32 devices in a mesh: row: 4 (over y, core), col: 8 (over z, x).
Axes of the slice: x: 2, y: 2, z: 4, core: 2. Of those that a mesh axis runs over, the one named last changes fastest.
Arguments:
- tile_values: bfloat16 [4, 8, 96, 256, 256], P('row', 'col')
- tile_index: int32 [4, 8, 96, 2], P('row', 'col'), may hold values from 0 to 15, as said below
- tile_count: int32 [4, 8], P('row', 'col'), may hold values from 12 to 96, as said below
- start_vectors: float32 [64, 16, 256], P(('row', 'col')), may hold values from -6 to 6
Outputs:
- iterate: float32 [64, 16, 256], P(('row', 'col'))
The draws below stay inside these ranges and needn't reach their ends.
Inputs may be any that keep to these rules, and one draw needn't show every extreme that they name: `tile_index`: on device (r, c), slot t holds a local block row in 0 .. 15 and a local block column in 0 .. 7; the pairs of the slots below tile_count[r, c] are distinct; slots at or beyond the count are to be ignored. `tile_count`: some device uses all 96 slots.
All inputs are finite; a program needn't handle non-finite values.
Results may differ from the reference program's by a relative error of at most 0.0075.
Values may be sent and summed in bfloat16 or wider, within the bound.
A program may use at most 64 MiB of HBM per device.

```python
import math
import jax
import jax.numpy as jnp
from jax import lax

B = 256
K = 16
PB = 2
MAXT = 96
ITERS = 5
NBLK = 64
N_ROW = 4
N_COL = 8


def tile_layout(key):
    key_levels, key_full, key_perm = jax.random.split(jax.random.fold_in(key, 11), 3)
    devices_all = N_ROW * N_COL
    levels = jax.random.randint(key_levels, (devices_all,), 0, 4)
    counts = jnp.right_shift(jnp.full((devices_all,), MAXT, jnp.int32), levels.astype(jnp.int32))
    chosen = jax.random.randint(key_full, (), 0, devices_all)
    counts = jnp.where(jnp.arange(devices_all) == chosen, MAXT, counts)
    grid = N_COL * PB * (N_ROW * PB)
    keys = jax.random.split(key_perm, devices_all)
    picks = jax.vmap(lambda one_key: jax.random.permutation(one_key, grid)[:MAXT])(keys)
    rows = picks // (N_ROW * PB)
    cols = picks % (N_ROW * PB)
    layout = jnp.stack([rows, cols], -1).reshape(N_ROW, N_COL, MAXT, 2).astype(jnp.int32)
    return (layout, counts.reshape(N_ROW, N_COL).astype(jnp.int32))


def draw_tile_index(key, part):
    layout, counts = tile_layout(key)
    return layout


def draw_tile_count(key, part):
    layout, counts = tile_layout(key)
    return counts


def draw_tile_values(key, part):
    key_base, key_rows = jax.random.split(jax.random.fold_in(key, 23), 2)
    shape = (N_ROW, N_COL, MAXT, B, B)
    sigma = (B * MAXT / (2.0 * PB)) ** (-0.5)
    trend = 3.0 ** (jnp.arange(N_ROW, dtype=jnp.float32) / (N_ROW - 1))
    trend = trend.reshape(N_ROW, 1, 1, 1, 1)
    row_factor = jnp.exp(jax.random.uniform(key_rows, (N_ROW, N_COL, MAXT, B, 1), jnp.float32, 0.0, math.log(4.0)))
    base = jax.random.normal(key_base, shape, jnp.float32)
    values = base * sigma * trend * row_factor
    return values.astype(jnp.bfloat16)


def level_of(own_key, extent, cuts, least, top_value):
    def one(axis_at, blocks):
        draws = jax.random.uniform(jax.random.fold_in(jax.random.fold_in(own_key, 6), axis_at), (blocks,), jnp.float32, least / len(cuts), top_value / len(cuts))
        return jnp.repeat(jnp.exp(draws), extent[axis_at] // blocks).reshape((-1,) + (1,) * (len(extent) - axis_at - 1))

    gain = one(*cuts[0])
    for cut in cuts[1:]:
        gain = gain * one(*cut)
    return gain


def gaussian(key, dims, spread, bound, cuts=(), kind=jnp.bfloat16):
    entries = spread * jax.random.normal(key, dims, jnp.float32)
    if cuts:
        entries = entries * level_of(key, dims, cuts, -0.22, 0.18)
    return jnp.clip(entries, -bound, bound).astype(kind)


def setup_inputs(seed: int = 0) -> dict:
    streams_of = jax.random.split(jax.random.key(seed), 5)
    tile_values = draw_tile_values(jax.random.fold_in(streams_of[4], 71), 0)
    tile_index = draw_tile_index(jax.random.fold_in(streams_of[4], 71), 0)
    tile_count = draw_tile_count(jax.random.fold_in(streams_of[4], 71), 0)
    start_vectors = gaussian(streams_of[3], (NBLK, K, B), 1.0, 6.0, ((0, 32),), jnp.float32)
    return {"tile_values": tile_values, "tile_index": tile_index, "tile_count": tile_count, "start_vectors": start_vectors}


epsilon = 1e-06

def reference(tile_values, tile_index, tile_count, start_vectors):
    row_blocks = N_COL * PB
    devices_all = N_ROW * N_COL
    flat_tiles = tile_values.reshape(devices_all, MAXT, B, B)
    flat_index = tile_index.reshape(devices_all, MAXT, 2)
    flat_count = tile_count.reshape(devices_all)
    device_ids = jnp.arange(devices_all, dtype=jnp.int32)
    row_device = device_ids // N_COL
    col_device = device_ids % N_COL
    global_rows = (row_device[:, None] * row_blocks + flat_index[:, :, 0]).astype(jnp.int32)
    local_cols = flat_index[:, :, 1]
    global_cols = ((local_cols // PB * N_COL + col_device[:, None]) * PB + local_cols % PB).astype(jnp.int32)
    slot_ids = jnp.arange(MAXT, dtype=jnp.int32)
    in_use = (slot_ids[None, :] < flat_count[:, None]).astype(jnp.float32)
    positions = NBLK * B
    current = start_vectors
    for iteration in range(ITERS):
        rounded = current.astype(jnp.bfloat16)
        rms = jnp.sqrt(lax.optimization_barrier(jnp.sum(current * current, axis=(0, 2))) / positions + epsilon)

        def one_device(accumulated, pieces):
            block_tiles, rows, cols, weights = pieces
            picked = jnp.take(rounded, cols, axis=0).astype(jnp.float32)
            products = jnp.einsum('tkb,tab->tka', picked, block_tiles.astype(jnp.float32))
            products = products * weights[:, None, None]
            return (accumulated.at[rows].add(products), None)
        accumulated, unused = lax.scan(one_device, jnp.zeros((NBLK, K, B), jnp.float32), (flat_tiles, global_rows, global_cols, in_use))
        current = accumulated / rms[None, :, None]
    return current
```

```python
import functools

import jax
import jax.numpy as jnp
from jax import lax
from jax.experimental import pallas as pl
from jax.experimental.pallas import tpu as pltpu
from jax.sharding import PartitionSpec as P

ITERS = 5
epsilon = 1e-06
MESH = pl.DeviceIdType.MESH
BF16 = jnp.bfloat16
F32 = jnp.float32


def largest_divisor(number, limit):
    return max(d for d in range(1, limit + 1) if number % d == 0)


def kernel(
    n_row, n_col, positions, chunk, dense,
    tiles_hbm, cols_ref, table_ref, start_ref, out_ref,
    tiles, flipped, prods, eye, held, v_all, send, rs, own, s_out, s_all,
    tile_sem, ag_send, ag_recv, s_send, s_recv, p_send, p_recv,
):
    capacity, size, _ = tiles.shape
    blocks, vectors, _ = start_ref.shape
    local_cols = n_row * blocks
    r = lax.axis_index("row")
    c = lax.axis_index("col")

    def load(g):
        span = pl.ds(g * chunk, chunk)
        return pltpu.make_async_copy(tiles_hbm.at[0, 0, span], tiles.at[span], tile_sem.at[g])

    for g in range(capacity // chunk):
        load(g).start()

    barrier = pltpu.get_barrier_semaphore()
    for d in range(1, n_row):
        pl.semaphore_signal(barrier, inc=1, device_id={"row": lax.rem(r + d, n_row)}, device_id_type=MESH)
    for d in range(1, n_col):
        pl.semaphore_signal(barrier, inc=1, device_id={"col": lax.rem(c + d, n_col)}, device_id_type=MESH)

    eye[...] = (
        lax.broadcasted_iota(jnp.int32, (size, size), 0) == lax.broadcasted_iota(jnp.int32, (size, size), 1)
    ).astype(F32).astype(BF16)
    prods[capacity] = jnp.zeros((vectors, size), F32)
    flipped[capacity] = jnp.zeros((size, size), BF16)
    diagonal = (
        lax.broadcasted_iota(jnp.int32, (vectors, 128), 0) == lax.broadcasted_iota(jnp.int32, (vectors, 128), 1)
    ).astype(F32)
    pl.semaphore_wait(barrier, n_row + n_col - 2)

    def gather_copy(par, d, source):
        return pltpu.make_async_remote_copy(
            src_ref=v_all.at[par, pl.ds(r * blocks, blocks)],
            dst_ref=v_all.at[par, pl.ds(source * blocks, blocks)],
            send_sem=ag_send.at[d],
            recv_sem=ag_recv.at[par, source],
            device_id={"row": lax.rem(r + d, n_row)},
            device_id_type=MESH,
        )

    def square_copy(par, d, source):
        return pltpu.make_async_remote_copy(
            src_ref=s_out,
            dst_ref=s_all.at[par, source],
            send_sem=s_send.at[d],
            recv_sem=s_recv.at[par, source],
            device_id={"col": lax.rem(c + d, n_col)},
            device_id_type=MESH,
        )

    def part_copy(par, d, source):
        return pltpu.make_async_remote_copy(
            src_ref=send.at[d],
            dst_ref=rs.at[par, source],
            send_sem=p_send.at[d],
            recv_sem=p_recv.at[par, source],
            device_id={"col": lax.rem(c + d, n_col)},
            device_id_type=MESH,
        )

    def share(par, current):
        v_all[par, pl.ds(r * blocks, blocks)] = current.astype(BF16)
        for d in range(1, n_row):
            gather_copy(par, d, r).start()
        for d in range(1, n_row):
            gather_copy(par, d, lax.rem(r + d, n_row)).wait_recv()
        held[...] = v_all[par]
        wide = held[...].astype(F32)
        squares = jnp.sum(wide * wide, axis=0)
        column = jnp.sum(squares, axis=1, keepdims=True)
        row = jnp.sum(column * diagonal, axis=0, keepdims=True)
        s_out[...] = row
        s_all[par, c] = row
        for d in range(1, n_col):
            square_copy(par, d, c).start()

    def looked_up(target, p, j):
        return table_ref[(target * blocks + p) * local_cols + j]

    def sum_products(target, p):
        total = prods[looked_up(target, p, 0)]
        for j in range(1, local_cols):
            total = total + prods[looked_up(target, p, j)]
        return total

    def exchange(par, row_sum, unrolled):
        def one(d):
            target = lax.rem(c + d, n_col)
            for p in range(blocks):
                send[d, p] = row_sum(target, p).astype(BF16)
            part_copy(par, d, c).start()

        if unrolled:
            for d in range(n_col - 1, 0, -1):
                one(d)
        else:
            @pl.loop(1, n_col)
            def _(d):
                one(d)

        for p in range(blocks):
            own[p] = row_sum(c, p)

    def finish(par):
        for d in range(1, n_col):
            square_copy(par, d, lax.rem(c + d, n_col)).wait_recv()
        squares = jnp.sum(s_all[par], axis=0)
        column = jnp.sum(squares * diagonal, axis=1, keepdims=True)
        rms = jnp.sqrt(column / positions + epsilon)
        total = own[...]
        for d in range(1, n_col):
            source = lax.rem(c + d, n_col)
            part_copy(par, d, source).wait_recv()
            total = total + rs[par, source].astype(F32)
        for d in range(1, n_row):
            gather_copy(par, d, r).wait_send()
        for d in range(1, n_col):
            square_copy(par, d, c).wait_send()
            part_copy(par, d, c).wait_send()
        out_ref[...] = total / rms[None]

    share(0, start_ref[...])

    @pl.loop(0, capacity // chunk)
    def _(g):
        load(g).wait()
        for u in range(chunk):
            t = g * chunk + u
            rows = jnp.concatenate([held[cols_ref[t]], eye[...]], axis=0)
            both = lax.dot_general(rows, tiles[t], (((1,), (1,)), ((), ())), preferred_element_type=F32)
            prods[t] = both[:vectors]
            flipped[t] = both[vectors:].astype(BF16)

    exchange(0, sum_products, n_col <= 8)
    finish(0)

    @pl.loop(1, ITERS)
    def _(step):
        par = lax.rem(step, 2)
        share(par, out_ref[...])
        if dense:
            def row_product(target, p):
                total = None
                for j in range(local_cols):
                    term = jnp.dot(held[j], flipped[looked_up(target, p, j)], preferred_element_type=F32)
                    total = term if total is None else total + term
                return total

            exchange(par, row_product, True)
        else:
            @pl.loop(0, capacity // chunk)
            def _(g):
                for u in range(chunk):
                    t = g * chunk + u
                    prods[t] = jnp.dot(held[cols_ref[t]], flipped[t], preferred_element_type=F32)

            exchange(par, sum_products, n_col <= 8)
        finish(par)


def shards(tile_values, tile_index, tile_count, start_vectors):
    n_row, n_col = lax.axis_size("row"), lax.axis_size("col")
    capacity, size = tile_values.shape[2], tile_values.shape[3]
    blocks, vectors, _ = start_vectors.shape
    rows_here, cols_here = n_col * blocks, n_row * blocks
    positions = n_row * n_col * blocks * size
    pairs = rows_here * cols_here
    layout = tile_index[0, 0]
    slots = jnp.arange(capacity, dtype=jnp.int32)
    cells = layout[:, 0] * cols_here + layout[:, 1]
    hit = (jnp.arange(pairs, dtype=jnp.int32)[:, None] == cells[None, :]) & (slots < tile_count[0, 0])[None, :]
    table = capacity + jnp.sum(jnp.where(hit, slots[None, :] - capacity, 0), axis=1)
    chunk = largest_divisor(capacity, 8)
    dense = pairs <= 2 * capacity
    vmem = pl.BlockSpec(memory_space=pltpu.VMEM)
    smem = pl.BlockSpec(memory_space=pltpu.SMEM)
    dma = pltpu.SemaphoreType.DMA
    return pl.pallas_call(
        functools.partial(kernel, n_row, n_col, positions, chunk, dense),
        out_shape=jax.ShapeDtypeStruct(start_vectors.shape, F32),
        in_specs=[pl.BlockSpec(memory_space=pl.ANY), smem, smem, vmem],
        out_specs=vmem,
        scratch_shapes=[
            pltpu.VMEM((capacity, size, size), BF16),
            pltpu.VMEM((capacity + 1, size, size), BF16),
            pltpu.VMEM((capacity + 1, vectors, size), F32),
            pltpu.VMEM((size, size), BF16),
            pltpu.VMEM((cols_here, vectors, size), BF16),
            pltpu.VMEM((2, cols_here, vectors, size), BF16),
            pltpu.VMEM((n_col, blocks, vectors, size), BF16),
            pltpu.VMEM((2, n_col, blocks, vectors, size), BF16),
            pltpu.VMEM((blocks, vectors, size), F32),
            pltpu.VMEM((1, 128), F32),
            pltpu.VMEM((2, n_col, 1, 128), F32),
            dma((capacity // chunk,)),
            dma((n_row,)),
            dma((2, n_row)),
            dma((n_col,)),
            dma((2, n_col)),
            dma((n_col,)),
            dma((2, n_col)),
        ],
        compiler_params=pltpu.CompilerParams(
            collective_id=0, has_side_effects=True, vmem_limit_bytes=48 * 1024 * 1024
        ),
    )(tile_values, layout[:, 1], table, start_vectors)


def solution(mesh):
    return jax.shard_map(
        shards,
        mesh=mesh,
        in_specs=(
            P("row", "col", None, None, None),
            P("row", "col", None, None),
            P("row", "col"),
            P(("row", "col"), None, None),
        ),
        out_specs=P(("row", "col"), None, None),
        check_vma=False,
    )
```

```python
import functools

import jax
import jax.numpy as jnp
from jax import lax
from jax.experimental import pallas as pl
from jax.experimental.pallas import tpu as pltpu
from jax.sharding import PartitionSpec as P

ITERS = 5
epsilon = 1e-06
CHUNK = 12
EARLY = 1
READY = 2
MESH = pl.DeviceIdType.MESH
BF16 = jnp.bfloat16
F32 = jnp.float32


def largest_divisor(number, limit):
    return max(d for d in range(1, limit + 1) if number % d == 0)


def row_order(r, n_row):
    partner = r + 1 - 2 * lax.rem(r, 2) if n_row % 2 == 0 else lax.rem(r + 1, n_row)
    base = r - lax.rem(r, 2) if n_row % 2 == 0 else r
    first = [r, partner]
    return first + [lax.rem(base + d, n_row) for d in range(2, n_row)]


def col_peer(c, d, n_col):
    if n_col & (n_col - 1):
        return lax.rem(c + d, n_col)
    peer, bit = 0, 1
    while bit < n_col:
        digit = lax.rem(c // bit, 2)
        peer = peer + bit * (1 - digit if d & bit else digit)
        bit *= 2
    return peer


def kernel(
    n_row, n_col, positions, chunk, early, dense,
    tiles_hbm, index_hbm, count_hbm, start_hbm, out_ref,
    tiles, flipped, prods, eye, held, v_all, send, rs, own, s_out, s_all,
    index_v, cols_ref, count_ref, start_v, table_v, table_ref,
    tile_sem, small_sem, ag_send, ag_recv, s_send, s_recv, p_send, p_recv,
):
    capacity, size, _ = tiles.shape
    blocks, vectors, _ = out_ref.shape
    local_cols = n_row * blocks
    r = lax.axis_index("row")
    c = lax.axis_index("col")

    start_copy = pltpu.make_async_copy(start_hbm, start_v, small_sem.at[0])
    index_copy = pltpu.make_async_copy(index_hbm, index_v, small_sem.at[1])
    count_copy = pltpu.make_async_copy(count_hbm, count_ref, small_sem.at[2])
    cols_copy = pltpu.make_async_copy(index_hbm, cols_ref, small_sem.at[3])
    start_copy.start()
    index_copy.start()
    count_copy.start()
    cols_copy.start()

    def load(g):
        span = pl.ds(g * chunk, chunk)
        return pltpu.make_async_copy(tiles_hbm.at[0, 0, span], tiles.at[span], tile_sem.at[g])

    for g in range(capacity // chunk):
        load(g).start()

    barrier = pltpu.get_barrier_semaphore()
    for d in range(1, n_row):
        pl.semaphore_signal(barrier, inc=1, device_id={"row": lax.rem(r + d, n_row)}, device_id_type=MESH)
    for d in range(1, n_col):
        pl.semaphore_signal(barrier, inc=1, device_id={"col": col_peer(c, d, n_col)}, device_id_type=MESH)

    eye[...] = (
        lax.broadcasted_iota(jnp.int32, (size, size), 0) == lax.broadcasted_iota(jnp.int32, (size, size), 1)
    ).astype(F32).astype(BF16)
    if not dense:
        prods[capacity] = jnp.zeros((vectors, size), F32)
    flipped[capacity] = jnp.zeros((size, size), BF16)
    diagonal = (
        lax.broadcasted_iota(jnp.int32, (vectors, 128), 0) == lax.broadcasted_iota(jnp.int32, (vectors, 128), 1)
    ).astype(F32)

    def flip(low, high):
        @pl.loop(low, high)
        def _(g):
            load(g).wait()
            for u in range(chunk):
                t = g * chunk + u
                if u % 3 == 2:
                    flipped[t] = tiles[t].T
                else:
                    flipped[t] = lax.dot_general(
                        eye[...], tiles[t], (((1,), (1,)), ((), ())), preferred_element_type=F32
                    ).astype(BF16)

    def gather_copy(par, d, source):
        return pltpu.make_async_remote_copy(
            src_ref=v_all.at[par, pl.ds(r * blocks, blocks)],
            dst_ref=v_all.at[par, pl.ds(source * blocks, blocks)],
            send_sem=ag_send.at[d],
            recv_sem=ag_recv.at[par, source],
            device_id={"row": row_order(r, n_row)[d]},
            device_id_type=MESH,
        )

    def square_copy(par, d, source):
        return pltpu.make_async_remote_copy(
            src_ref=s_out,
            dst_ref=s_all.at[par, source],
            send_sem=s_send.at[d],
            recv_sem=s_recv.at[par, source],
            device_id={"col": col_peer(c, d, n_col)},
            device_id_type=MESH,
        )

    def part_copy(par, d, source):
        return pltpu.make_async_remote_copy(
            src_ref=send.at[d],
            dst_ref=rs.at[par, source],
            send_sem=p_send.at[d],
            recv_sem=p_recv.at[par, source],
            device_id={"col": col_peer(c, d, n_col)},
            device_id_type=MESH,
        )

    def share(par, current):
        v_all[par, pl.ds(r * blocks, blocks)] = current.astype(BF16)
        for d in range(1, n_row):
            gather_copy(par, d, r).start()

    def arrive(par, n):
        gather_copy(par, n, row_order(r, n_row)[n]).wait_recv()

    def total_squares(par):
        held[...] = v_all[par]
        wide = held[...].astype(F32)
        squares = jnp.sum(wide * wide, axis=0)
        column = jnp.sum(squares, axis=1, keepdims=True)
        row = jnp.sum(column * diagonal, axis=0, keepdims=True)
        s_out[...] = row
        s_all[par, c] = row
        for d in range(1, n_col):
            square_copy(par, d, c).start()

    def looked_up(target, p, j):
        cell = (target * blocks + p) * local_cols + j
        return table_ref[cell // 128, cell % 128]

    def sum_products(target, p):
        total = prods[looked_up(target, p, 0)]
        for j in range(1, local_cols):
            total = total + prods[looked_up(target, p, j)]
        return total

    def exchange(par, row_sum, unrolled):
        def one(d):
            target = col_peer(c, d, n_col)
            for p in range(blocks):
                send[d, p] = row_sum(target, p).astype(BF16)
            part_copy(par, d, c).start()

        if unrolled:
            for d in range(n_col - 1, 0, -1):
                one(d)
        else:
            for d in range(n_col - 1, 0, -1):
                one(d)

        for p in range(blocks):
            own[p] = row_sum(c, p)

    def finish(par):
        for d in range(1, n_col):
            square_copy(par, d, col_peer(c, d, n_col)).wait_recv()
        squares = jnp.sum(s_all[par], axis=0)
        column = jnp.sum(squares * diagonal, axis=1, keepdims=True)
        rms = jnp.sqrt(column / positions + epsilon)
        total = own[...]
        for d in range(1, n_col):
            source = col_peer(c, d, n_col)
            part_copy(par, d, source).wait_recv()
            total = total + rs[par, source].astype(F32)
        for d in range(1, n_row):
            gather_copy(par, d, r).wait_send()
        for d in range(1, n_col):
            square_copy(par, d, c).wait_send()
            part_copy(par, d, c).wait_send()
        out_ref[...] = total / rms[None]

    start_copy.wait()
    index_copy.wait()
    count_copy.wait()
    cols_copy.wait()
    slots = lax.broadcasted_iota(jnp.int32, (1, capacity), 1)
    cells = index_v[0:1, :] * local_cols + index_v[1:2, :]
    cells = jnp.where(slots < count_ref[0, 0], cells, -1)
    pair = lax.broadcasted_iota(jnp.int32, (128, 1), 0)
    on_diagonal = lax.broadcasted_iota(jnp.int32, (128, 128), 0) == lax.broadcasted_iota(jnp.int32, (128, 128), 1)
    for q in range(table_v.shape[0]):
        found = jnp.sum(jnp.where(pair + q * 128 == cells, slots - capacity, 0), axis=1, keepdims=True)
        table_v[q : q + 1, :] = capacity + jnp.sum(jnp.where(on_diagonal, found, 0), axis=0, keepdims=True)
    table_copy = pltpu.make_async_copy(table_v, table_ref, small_sem.at[4])
    table_copy.start()

    flip(0, early)
    pl.semaphore_wait(barrier, n_row + n_col - 2)
    share(0, start_v[...])
    flip(early, capacity // chunk)
    table_copy.wait()

    @pl.loop(0, ITERS)
    def _(step):
        par = lax.rem(step, 2)
        if dense:
            def add(total, source, target, p):
                for j in range(blocks):
                    term = jnp.dot(
                        v_all[par, source * blocks + j],
                        flipped[looked_up(target, p, source * blocks + j)],
                        preferred_element_type=F32,
                    )
                    total = term if total is None else total + term
                return total

            sources = row_order(r, n_row)
            for n, source in enumerate(sources[:-READY]):
                if n:
                    arrive(par, n)
                for i in range(n_col):
                    for p in range(blocks):
                        prods[i * blocks + p] = add(prods[i * blocks + p] if n else None, source, i, p)
            for n in range(n_row - READY, n_row):
                arrive(par, n)
            total_squares(par)

            def row_product(target, p):
                total = prods[target * blocks + p]
                for source in sources[-READY:]:
                    total = add(total, source, target, p)
                return total

            exchange(par, row_product, True)
        else:
            for n in range(1, n_row):
                arrive(par, n)
            total_squares(par)

            @pl.loop(0, capacity // chunk)
            def _(g):
                for u in range(chunk):
                    t = g * chunk + u
                    prods[t] = jnp.dot(held[cols_ref[1, t]], flipped[t], preferred_element_type=F32)

            exchange(par, sum_products, n_col <= 8)
        finish(par)

        @pl.when(step < ITERS - 1)
        def _():
            share(1 - par, out_ref[...])


def shards(tile_values, tile_index, tile_count, start_vectors):
    n_row, n_col = lax.axis_size("row"), lax.axis_size("col")
    capacity, size = tile_values.shape[2], tile_values.shape[3]
    blocks, vectors, _ = start_vectors.shape
    rows_here, cols_here = n_col * blocks, n_row * blocks
    positions = n_row * n_col * blocks * size
    pairs = rows_here * cols_here
    chunk = largest_divisor(capacity, CHUNK)
    early = min(EARLY, capacity // chunk)
    dense = pairs <= 2 * capacity
    vmem = pl.BlockSpec(memory_space=pltpu.VMEM)
    dma = pltpu.SemaphoreType.DMA
    return pl.pallas_call(
        functools.partial(kernel, n_row, n_col, positions, chunk, early, dense),
        out_shape=jax.ShapeDtypeStruct(start_vectors.shape, F32),
        in_specs=[pl.BlockSpec(memory_space=pltpu.HBM)] * 4,
        out_specs=vmem,
        scratch_shapes=[
            pltpu.VMEM((capacity, size, size), BF16),
            pltpu.VMEM((capacity + 1, size, size), BF16),
            pltpu.VMEM((rows_here if dense else capacity + 1, vectors, size), F32),
            pltpu.VMEM((size, size), BF16),
            pltpu.VMEM((cols_here, vectors, size), BF16),
            pltpu.VMEM((2, cols_here, vectors, size), BF16),
            pltpu.VMEM((n_col, blocks, vectors, size), BF16),
            pltpu.VMEM((2, n_col, blocks, vectors, size), BF16),
            pltpu.VMEM((blocks, vectors, size), F32),
            pltpu.VMEM((1, 128), F32),
            pltpu.VMEM((2, n_col, 1, 128), F32),
            pltpu.VMEM((2, capacity), jnp.int32),
            pltpu.SMEM((2, capacity), jnp.int32),
            pltpu.SMEM((1, 1), jnp.int32),
            pltpu.VMEM(start_vectors.shape, F32),
            pltpu.VMEM((pl.cdiv(pairs, 128), 128), jnp.int32),
            pltpu.SMEM((pl.cdiv(pairs, 128), 128), jnp.int32),
            dma((capacity // chunk,)),
            dma((5,)),
            dma((n_row,)),
            dma((2, n_row)),
            dma((n_col,)),
            dma((2, n_col)),
            dma((n_col,)),
            dma((2, n_col)),
        ],
        compiler_params=pltpu.CompilerParams(
            collective_id=0, has_side_effects=True, vmem_limit_bytes=48 * 1024 * 1024
        ),
    )(tile_values, tile_index[0, 0].T, tile_count, start_vectors)


def solution(mesh):
    return jax.shard_map(
        shards,
        mesh=mesh,
        in_specs=(
            P("row", "col", None, None, None),
            P("row", "col", None, None),
            P("row", "col"),
            P(("row", "col"), None, None),
        ),
        out_specs=P(("row", "col"), None, None),
        check_vma=False,
    )
```
